512 devices in a mesh: section: 8 (over y_hi, core), dp: 64 (over x, y_lo, z).
Axes of the slice: x: 4, y: 8 (y_hi: 4, y_lo: 2; y = y_hi * 2 + y_lo), z: 8, core: 2. Of those that a mesh axis runs over, the one named last changes fastest.
Arguments:
- node_table: bfloat16 [128, 2048], replicated, may hold values from -60 to 60
- tiles: int32 [4, 2048], P(None, 'dp'), may hold values from 0 to 96
- neighbours: int32 [4, 2048, 8], P(None, 'dp'), may hold values from 0 to 31
- distances: float32 [4, 2048, 8], P(None, 'dp'), may hold values from 0 to 0.9
- proj: bfloat16 [8, 2048, 512], P('section'), may hold values from -0.125 to 0.125
- upstream: bfloat16 [4, 2048, 2048], P(None, 'dp'), may hold values from -16 to 16
Outputs:
- grad: float32 [8, 2048, 512], P('section', 'dp')
The draws below stay inside these ranges and needn't reach their ends.
All inputs are finite; a program needn't handle non-finite values.
Results may differ from the reference program's by a relative error of at most 0.024.
Values may be sent and summed in bfloat16 or wider, within the bound.
A program may use at most 64 MiB of HBM per device.

```python
import math
import jax
import jax.numpy as jnp
from jax import lax

D = 2048
RANK = 512
MICRO = 4
NODES = 128
LOCAL = 32
NEIGH = 8
SECTIONS = 8
POINTS = 2048


def draw_node_table(key, part):
    key_base = jax.random.fold_in(key, 11)
    key_values, key_rows, key_cols = jax.random.split(key_base, 3)
    row_scale = jnp.exp(jax.random.uniform(key_rows, (NODES, 1), jnp.float32, math.log(0.4), math.log(4.0)))
    col_scale = jnp.exp(jax.random.uniform(key_cols, (1, D), jnp.float32, math.log(0.5), math.log(2.0)))
    values = jax.random.normal(key_values, (NODES, D), jnp.float32)
    table = jnp.clip(values * row_scale * col_scale, -60.0, 60.0)
    return table.astype(jnp.bfloat16)


def with_ends(drawn, key, least, high):
    index_at = [jax.random.randint(jax.random.fold_in(key, axis), (), 0, length) for axis, length in enumerate(drawn.shape)]
    main_axis = drawn.shape.index(max(drawn.shape))
    next_to = index_at[:main_axis] + [(index_at[main_axis] + 1) % drawn.shape[main_axis]] + index_at[main_axis + 1:]
    return drawn.at[tuple(index_at)].set(least).at[tuple(next_to)].set(high)


def with_spikes(entries, own_key, source, target, parts, factor):
    def block_of(axis_at):
        return (jnp.arange(entries.shape[axis_at]) // (entries.shape[axis_at] // parts)).reshape((-1,) + (1,) * (entries.ndim - 1 - axis_at))

    first = jax.random.permutation(own_key, parts)[block_of(target)]
    other_side = (block_of(target) + parts // 2) % parts
    return jnp.where((block_of(source) == first) | (block_of(source) == other_side), factor * entries, entries)


def levels(key, dims, cuts, low, high):
    factor_of = 1.0
    for position, parts in cuts:
        steps = jax.random.uniform(jax.random.fold_in(jax.random.fold_in(key, 6), position), (parts,), jnp.float32, low / len(cuts), high / len(cuts))
        factor_of = factor_of * jnp.repeat(jnp.exp(steps), dims[position] // parts).reshape((-1,) + (1,) * (len(dims) - 1 - position))
    return factor_of


def bell_draw(rng, dims, spread, reach, cuts=(), held_as=jnp.bfloat16):
    values = jax.random.normal(rng, dims, jnp.float32) * spread
    if len(cuts) > 0:
        values = levels(rng, dims, cuts, -0.22, 0.18) * values
    return jnp.clip(values, min=-reach, max=reach).astype(held_as)


def gaussian_with(rng, extent, scale, most, cuts, heavy, held_as=jnp.bfloat16):
    result = scale * jax.random.normal(rng, extent, jnp.float32)
    if cuts:
        result = result * levels(rng, extent, cuts, -0.22, 0.18)
    return jnp.clip(with_spikes(result, jax.random.fold_in(rng, 3), *heavy), -most, most).astype(held_as)


def setup_inputs(seed: int = 0) -> dict:
    seeds = jax.random.split(jax.random.key(seed), 7)
    node_table = draw_node_table(jax.random.fold_in(seeds[6], 71), 0)
    tiles = with_ends(jax.random.randint(seeds[1], (MICRO, POINTS), 0, NODES - LOCAL + 1), jax.random.fold_in(seeds[1], 1), 0, NODES - LOCAL).astype(jnp.int32)
    neighbours = with_ends(jax.random.randint(seeds[2], (MICRO, POINTS, NEIGH), 0, LOCAL), jax.random.fold_in(seeds[2], 1), 0, LOCAL - 1).astype(jnp.int32)
    distances = jnp.clip(0.9 * jax.random.uniform(seeds[3], (MICRO, POINTS, NEIGH), jnp.float32) ** levels(seeds[3], (MICRO, POINTS, NEIGH), ((1, 64),), -0.2, 0.2), 0.0, 0.9)
    proj = bell_draw(seeds[4], (SECTIONS, D, RANK), D ** -0.5, 0.125, ((0, 8),))
    upstream = gaussian_with(seeds[5], (MICRO, POINTS, D), 1.0, 16.0, ((1, 64),), (1, 2, 64, 4.0))
    return dict(node_table=node_table, tiles=tiles, neighbours=neighbours, distances=distances, proj=proj, upstream=upstream)


epsilon = 1e-05

def normalize(stream):
    wide = stream.astype(jnp.float32)
    inv_rms = lax.rsqrt(lax.optimization_barrier(jnp.mean(wide * wide, axis=-1, keepdims=True)) + epsilon)
    return (wide * inv_rms, inv_rms)

def contract_rows(left, right):
    return lax.dot_general(left, right, (((0,), (0,)), ((), ())), preferred_element_type=jnp.float32)

def contract_last(left, right):
    return lax.dot_general(left, right, (((1,), (1,)), ((), ())), preferred_element_type=jnp.float32)

def features(node_table, tile_row, neighbour_rows, distance_rows):
    kernel = (1.0 - distance_rows) ** 3 * (1.0 + 3.0 * distance_rows)
    weight_sum = lax.optimization_barrier(jnp.sum(kernel, axis=-1))
    node_index = (tile_row[:, None] + neighbour_rows).astype(jnp.int32)
    picked = jnp.take(node_table, node_index, axis=0).astype(jnp.float32)
    mixed = lax.optimization_barrier(jnp.sum(picked * kernel[:, :, None], axis=1)) / weight_sum[:, None]
    return mixed.astype(jnp.bfloat16)

def reference(node_table, tiles, neighbours, distances, proj, upstream):
    layers = proj.shape[0]

    def micro_step(totals, batch):
        tile_row, neighbour_rows, distance_rows, upstream_rows = batch
        stream = features(node_table, tile_row, neighbour_rows, distance_rows)
        inputs = []
        for layer in range(layers):
            inputs.append(stream)
            wide, inv_rms = normalize(stream)
            normed = wide.astype(jnp.bfloat16)
            hidden = jnp.tanh(jnp.dot(normed, proj[layer], preferred_element_type=jnp.float32)).astype(jnp.bfloat16)
            stream = (stream.astype(jnp.float32) + contract_last(hidden, proj[layer])).astype(jnp.bfloat16)
        grads = []
        cotangent = upstream_rows
        for layer in reversed(range(layers)):
            wide, inv_rms = normalize(inputs[layer])
            normed = wide.astype(jnp.bfloat16)
            hidden = jnp.tanh(jnp.dot(normed, proj[layer], preferred_element_type=jnp.float32)).astype(jnp.bfloat16)
            hidden_wide = hidden.astype(jnp.float32)
            grad_hidden = jnp.dot(cotangent, proj[layer], preferred_element_type=jnp.float32)
            grad_act = (grad_hidden * (1.0 - hidden_wide * hidden_wide)).astype(jnp.bfloat16)
            grad_norm = contract_last(grad_act, proj[layer])
            grads.append(contract_rows(normed, grad_act) + contract_rows(cotangent, hidden))
            correction = lax.optimization_barrier(jnp.mean(grad_norm * wide, axis=-1, keepdims=True))
            cotangent = (cotangent.astype(jnp.float32) + inv_rms * (grad_norm - wide * correction)).astype(jnp.bfloat16)
        return (totals + jnp.stack(grads[::-1]), None)
    zeros = jnp.zeros(proj.shape, jnp.float32)
    grad, _ = lax.scan(micro_step, zeros, (tiles, neighbours, distances, upstream))
    factor = 1.0 / math.sqrt(MICRO * POINTS)
    return grad * factor
```

```python
import functools
import math

import jax
import jax.numpy as jnp
from jax import lax
from jax.experimental import pallas as pl
from jax.experimental.pallas import tpu as pltpu
from jax.sharding import Mesh
from jax.sharding import PartitionSpec as P

DP = ("dp_0", "dp_1", "dp_2")
MESH = pl.DeviceIdType.MESH
EPSILON = 1e-05
STEP_ROWS = 16

f32 = jnp.float32
bf16 = jnp.bfloat16


def across_rows(left, right):
    return lax.dot_general(left, right, (((0,), (0,)), ((), ())), preferred_element_type=f32)


def kernel(
    factor,
    tiles,
    neighbours,
    distances,
    table_hbm,
    proj,
    upstream,
    out,
    table,
    weight,
    flip,
    stage,
    ahead,
    behind,
    inv_rms,
    cols,
    acts,
    partial,
    z_in,
    y_out,
    y_in,
    ahead_send,
    ahead_recv,
    behind_send,
    behind_recv,
    x_send,
    x_recv,
    z_send,
    z_recv,
    y_send,
    y_recv,
    load_sem,
):
    sections = lax.axis_size("section")
    xs, ys, zs = (lax.axis_size(a) for a in DP)
    section = lax.axis_index("section")
    x, y, z = (lax.axis_index(a) for a in DP)
    rows, width = upstream.shape
    micro, near, points = neighbours.shape
    steps = rows // STEP_ROWS
    slab = width // xs
    first, last = section == 0, section == sections - 1

    load_weight = pltpu.make_async_copy(proj.at[0], weight, load_sem.at[0])
    load_table = pltpu.make_async_copy(table_hbm, table, load_sem.at[1])
    load_upstream = pltpu.make_async_copy(
        upstream, stage.at[pl.ds(rows, rows)], load_sem.at[2]
    )
    load_weight.start()

    @pl.when(first)
    def _():
        load_table.start()

    @pl.when(last)
    def _():
        load_upstream.start()

    barrier = pltpu.get_barrier_semaphore()

    def greet(where):
        pl.semaphore_signal(barrier, inc=1, device_id=where, device_id_type=MESH)

    @pl.when(jnp.logical_not(first))
    def _():
        greet({"section": section - 1})

    @pl.when(jnp.logical_not(last))
    def _():
        greet({"section": section + 1})

    for d in range(1, xs):
        greet({"dp_0": lax.rem(x + d, xs)})
    for d in range(1, ys):
        greet({"dp_1": lax.rem(y + d, ys)})
    for d in range(1, zs):
        greet({"dp_2": lax.rem(z + d, zs)})

    @pl.when(first)
    def _():
        nodes = lax.broadcasted_iota(jnp.int32, (table.shape[0], points), 0)
        load_table.wait()
        for i in range(micro):
            r = distances[i]
            kernel_values = (1.0 - r) ** 3 * (1.0 + 3.0 * r)
            total = jnp.sum(kernel_values, axis=0, keepdims=True)
            index = tiles[i : i + 1, :] + neighbours[i]
            selector = jnp.zeros(nodes.shape, f32)
            for k in range(near):
                selector += jnp.where(index[k : k + 1] == nodes, kernel_values[k : k + 1], 0.0)
            selector = selector / total
            high = selector.astype(bf16)
            low = (selector - high.astype(f32)).astype(bf16)
            mixed = across_rows(high, table[...]) + across_rows(low, table[...])
            stage[i * points : (i + 1) * points, :] = mixed.astype(bf16)

    @pl.when(last)
    def _():
        load_upstream.wait()

    load_weight.wait()
    flip[...] = weight[...].T

    ends = jnp.where(jnp.logical_or(first, last), 1, 2)
    pl.semaphore_wait(barrier, xs + ys + zs - 3 + ends)

    def block(m, base=0):
        return pl.ds(pl.multiple_of(base + m * STEP_ROWS, STEP_ROWS), STEP_ROWS)

    def to_ahead(src, dst, sem):
        return pltpu.make_async_remote_copy(
            src_ref=src,
            dst_ref=dst,
            send_sem=ahead_send,
            recv_sem=sem,
            device_id={"section": lax.rem(section + 1, sections)},
            device_id_type=MESH,
        )

    def to_behind(src, dst, sem):
        return pltpu.make_async_remote_copy(
            src_ref=src,
            dst_ref=dst,
            send_sem=behind_send,
            recv_sem=sem,
            device_id={"section": lax.rem(section + sections - 1, sections)},
            device_id_type=MESH,
        )

    def ahead_copy(m):
        return to_ahead(ahead.at[block(m)], stage.at[block(m)], ahead_recv.at[m])

    def behind_copy(m):
        return to_behind(behind.at[block(m)], stage.at[block(m, rows)], behind_recv.at[m])

    def x_copy(kind, d, src, dst):
        return pltpu.make_async_remote_copy(
            src_ref=src,
            dst_ref=dst,
            send_sem=x_send.at[kind, d - 1],
            recv_sem=x_recv.at[kind, d - 1],
            device_id={"dp_0": lax.rem(x + d, xs)},
            device_id_type=MESH,
        )

    def share(m, half, act_half):
        for d in range(1, xs):
            to = lax.rem(x + d, xs)
            lanes = pl.ds(pl.multiple_of(to * slab, slab), slab)
            x_copy(
                2 * half,
                d,
                stage.at[block(m, half * rows), lanes],
                cols.at[block(m, (2 * d + half) * rows)],
            ).start()
            x_copy(
                2 * half + 1,
                d,
                acts.at[block(m, act_half * rows)],
                acts.at[block(m, (2 * d + act_half) * rows)],
            ).start()

    def forward(m):
        @pl.when(jnp.logical_not(first))
        def _():
            ahead_copy(m).wait_recv()

        stream = stage[block(m), :].astype(f32)
        inv = lax.rsqrt(jnp.mean(stream * stream, axis=-1, keepdims=True) + EPSILON)
        inner = jnp.dot(stage[block(m), :], weight[...], preferred_element_type=f32)
        hidden = jnp.tanh(inner * inv).astype(bf16)
        acts[block(m, rows), :] = hidden
        inv_rms[block(m), :] = jnp.broadcast_to(inv, (STEP_ROWS, 128))

        @pl.when(jnp.logical_not(last))
        def _():
            grown = stream + jnp.dot(hidden, flip[...], preferred_element_type=f32)
            ahead[block(m), :] = grown.astype(bf16)
            ahead_copy(m).start()

        share(m, 0, 1)

    def backward(m):
        @pl.when(jnp.logical_not(last))
        def _():
            behind_copy(m).wait_recv()

        cot = stage[block(m, rows), :]
        hidden = acts[block(m, rows), :].astype(f32)
        inv = inv_rms[block(m), 0:1]
        act_grad = jnp.dot(cot, weight[...], preferred_element_type=f32) * (1.0 - hidden * hidden)
        acts[block(m), :] = (act_grad * inv).astype(bf16)

        @pl.when(jnp.logical_not(first))
        def _():
            norm_grad = jnp.dot(act_grad.astype(bf16), flip[...], preferred_element_type=f32)
            wide = stage[block(m), :].astype(f32) * inv
            correction = jnp.mean(norm_grad * wide, axis=-1, keepdims=True)
            shrunk = cot.astype(f32) + inv * (norm_grad - wide * correction)
            behind[block(m), :] = shrunk.astype(bf16)
            behind_copy(m).start()

        share(m, 1, 0)

    lead = jnp.where(last, 1, jnp.where(section == sections - 2, 3, steps))

    def tick(t, carry):
        k = t - lead
        middle = jnp.logical_and(t >= lead, t < 2 * steps - lead)
        odd = lax.rem(k + 2 * steps, 2) == 1
        half = lax.div(k + 2 * steps, 2) - steps
        is_forward = jnp.logical_or(t < lead, jnp.logical_and(middle, odd))
        m_forward = jnp.where(t < lead, t, lead + half)
        m_backward = jnp.where(middle, half, t - steps)

        @pl.when(is_forward)
        def _():
            forward(m_forward)

        @pl.when(jnp.logical_not(is_forward))
        def _():
            backward(m_backward)

        return carry

    lax.fori_loop(0, 2 * steps, tick, 0)

    own = pl.ds(pl.multiple_of(x * slab, slab), slab)
    cols[0 : 2 * rows, :] = stage[:, own]

    def shared(kind, d):
        part = pl.ds((2 * d + (kind // 2 if kind % 2 == 0 else 1 - kind // 2)) * rows, rows)
        buffer = cols if kind % 2 == 0 else acts
        return x_copy(kind, d, buffer.at[part], buffer.at[part])

    for d in range(1, xs):
        for kind in range(4):
            shared(kind, d).wait_recv()
    local = across_rows(cols[...], acts[...])
    partial[...] = local.astype(bf16).reshape(partial.shape)

    def z_copy(d):
        to = lax.rem(z + d, zs)
        return pltpu.make_async_remote_copy(
            src_ref=partial.at[:, to],
            dst_ref=z_in.at[d - 1],
            send_sem=z_send.at[d - 1],
            recv_sem=z_recv.at[d - 1],
            device_id={"dp_2": to},
            device_id_type=MESH,
        )

    for d in range(1, zs):
        z_copy(d).start()
    summed = partial[:, z].astype(f32)
    for d in range(1, zs):
        z_copy(d).wait_recv()
        summed = summed + z_in[d - 1].astype(f32)
    y_out[...] = summed.astype(bf16)

    other = 1 - y
    y_copy = pltpu.make_async_remote_copy(
        src_ref=y_out.at[other],
        dst_ref=y_in,
        send_sem=y_send,
        recv_sem=y_recv,
        device_id={"dp_1": other},
        device_id_type=MESH,
    )
    y_copy.start()
    y_copy.wait_recv()
    out[0] = (y_out[y].astype(f32) + y_in[...].astype(f32)) * factor

    y_copy.wait_send()
    for d in range(1, zs):
        z_copy(d).wait_send()
    for d in range(1, xs):
        for kind in range(4):
            shared(kind, d).wait_send()

    @pl.when(jnp.logical_not(last))
    def _():
        to_ahead(ahead, stage.at[pl.ds(0, rows)], ahead_recv.at[0]).wait_send()

    @pl.when(jnp.logical_not(first))
    def _():
        to_behind(behind, stage.at[pl.ds(rows, rows)], behind_recv.at[0]).wait_send()


def on_device(node_table, tiles, neighbours, distances, proj, upstream):
    micro, points = tiles.shape
    rows = micro * points
    _, width, rank = proj.shape
    xs, ys, zs = (lax.axis_size(a) for a in DP)
    steps = rows // STEP_ROWS
    share = width // (xs * ys * zs)
    vmem = pl.BlockSpec(memory_space=pltpu.VMEM)
    hbm = pl.BlockSpec(memory_space=pltpu.HBM)
    dma = pltpu.SemaphoreType.DMA
    return pl.pallas_call(
        functools.partial(kernel, 1.0 / math.sqrt(rows * xs * ys * zs)),
        out_shape=jax.ShapeDtypeStruct((1, share, rank), f32),
        in_specs=[vmem] * 3 + [hbm] * 3,
        out_specs=vmem,
        scratch_shapes=[
            pltpu.VMEM(node_table.shape, bf16),
            pltpu.VMEM((width, rank), bf16),
            pltpu.VMEM((rank, width), bf16),
            pltpu.VMEM((2 * rows, width), bf16),
            pltpu.VMEM((rows, width), bf16),
            pltpu.VMEM((rows, width), bf16),
            pltpu.VMEM((rows, 128), f32),
            pltpu.VMEM((2 * xs * rows, width // xs), bf16),
            pltpu.VMEM((2 * xs * rows, rank), bf16),
            pltpu.VMEM((ys, zs, share, rank), bf16),
            pltpu.VMEM((zs - 1, ys, share, rank), bf16),
            pltpu.VMEM((ys, share, rank), bf16),
            pltpu.VMEM((share, rank), bf16),
            dma,
            dma((steps,)),
            dma,
            dma((steps,)),
            dma((4, xs - 1)),
            dma((4, xs - 1)),
            dma((zs - 1,)),
            dma((zs - 1,)),
            dma,
            dma,
            dma((3,)),
        ],
        compiler_params=pltpu.CompilerParams(
            collective_id=0, has_side_effects=True
        ),
    )(
        tiles,
        neighbours.transpose(0, 2, 1),
        distances.transpose(0, 2, 1),
        node_table,
        proj,
        upstream.reshape(rows, width),
    )


def solution(mesh):
    finer = Mesh(
        mesh.devices.reshape(mesh.shape["section"], 4, 2, 8), ("section", "dp_0", "dp_1", "dp_2")
    )
    in_specs = (
        P(),
        P(None, DP),
        P(None, DP, None),
        P(None, DP, None),
        P("section", None, None),
        P(None, DP, None),
    )
    out_specs = P("section", DP, None)
    return jax.shard_map(
        on_device, mesh=finer, in_specs=in_specs, out_specs=out_specs, check_vma=False
    )
```

```python
import functools
import math

import jax
import jax.numpy as jnp
from jax import lax
from jax.experimental import pallas as pl
from jax.experimental.pallas import tpu as pltpu
from jax.sharding import Mesh
from jax.sharding import PartitionSpec as P

DP = ("dp_0", "dp_1", "dp_2")
MESH = pl.DeviceIdType.MESH
EPSILON = 1e-05
STEP_ROWS = 16

f32 = jnp.float32
bf16 = jnp.bfloat16


def across_rows(left, right):
    return lax.dot_general(left, right, (((0,), (0,)), ((), ())), preferred_element_type=f32)


def kernel(
    factor,
    tiles,
    neighbours,
    distances,
    table_hbm,
    proj,
    upstream,
    out,
    table,
    weight,
    flip,
    stage,
    ahead,
    behind,
    inv_rms,
    cols,
    acts,
    partial,
    arrived,
    ahead_send,
    ahead_recv,
    behind_send,
    behind_recv,
    x_send,
    x_recv,
    plane_send,
    plane_recv,
    load_sem,
):
    sections = lax.axis_size("section")
    xs, ys, zs = (lax.axis_size(a) for a in DP)
    section = lax.axis_index("section")
    x, y, z = (lax.axis_index(a) for a in DP)
    rows, width = upstream.shape
    micro, near, points = neighbours.shape
    steps = rows // STEP_ROWS
    slab = width // xs
    first, last = section == 0, section == sections - 1

    load_weight = pltpu.make_async_copy(proj.at[0], weight, load_sem.at[0])
    load_table = pltpu.make_async_copy(table_hbm, table, load_sem.at[1])
    load_upstream = pltpu.make_async_copy(
        upstream, stage.at[pl.ds(rows, rows)], load_sem.at[2]
    )
    load_weight.start()

    @pl.when(first)
    def _():
        load_table.start()

    @pl.when(last)
    def _():
        load_upstream.start()

    barrier = pltpu.get_barrier_semaphore()

    def greet(where):
        pl.semaphore_signal(barrier, inc=1, device_id=where, device_id_type=MESH)

    @pl.when(jnp.logical_not(first))
    def _():
        greet({"section": section - 1})

    @pl.when(jnp.logical_not(last))
    def _():
        greet({"section": section + 1})

    for d in range(1, xs):
        greet({"dp_0": lax.rem(x + d, xs)})
    place = y * zs + z

    def plane(d):
        to = lax.rem(place + d, ys * zs)
        return to, {"dp_1": lax.div(to, zs), "dp_2": lax.rem(to, zs)}

    for d in range(1, ys * zs):
        greet(plane(d)[1])

    @pl.when(first)
    def _():
        nodes = lax.broadcasted_iota(jnp.int32, (table.shape[0], points), 0)
        load_table.wait()
        for i in range(micro):
            r = distances[i]
            kernel_values = (1.0 - r) ** 3 * (1.0 + 3.0 * r)
            total = jnp.sum(kernel_values, axis=0, keepdims=True)
            index = tiles[i : i + 1, :] + neighbours[i]
            selector = jnp.zeros(nodes.shape, f32)
            for k in range(near):
                selector += jnp.where(index[k : k + 1] == nodes, kernel_values[k : k + 1], 0.0)
            selector = selector / total
            high = selector.astype(bf16)
            low = (selector - high.astype(f32)).astype(bf16)
            mixed = across_rows(high, table[...]) + across_rows(low, table[...])
            stage[i * points : (i + 1) * points, :] = mixed.astype(bf16)

    @pl.when(last)
    def _():
        load_upstream.wait()

    load_weight.wait()
    flip[...] = weight[...].T

    ends = jnp.where(jnp.logical_or(first, last), 1, 2)
    pl.semaphore_wait(barrier, xs + ys * zs - 2 + ends)

    def block(m, base=0):
        return pl.ds(pl.multiple_of(base + m * STEP_ROWS, STEP_ROWS), STEP_ROWS)

    def to_ahead(src, dst, sem):
        return pltpu.make_async_remote_copy(
            src_ref=src,
            dst_ref=dst,
            send_sem=ahead_send,
            recv_sem=sem,
            device_id={"section": lax.rem(section + 1, sections)},
            device_id_type=MESH,
        )

    def to_behind(src, dst, sem):
        return pltpu.make_async_remote_copy(
            src_ref=src,
            dst_ref=dst,
            send_sem=behind_send,
            recv_sem=sem,
            device_id={"section": lax.rem(section + sections - 1, sections)},
            device_id_type=MESH,
        )

    def ahead_copy(m):
        return to_ahead(ahead.at[block(m)], stage.at[block(m)], ahead_recv.at[m])

    def behind_copy(m):
        return to_behind(behind.at[block(m)], stage.at[block(m, rows)], behind_recv.at[m])

    def x_copy(kind, d, src, dst):
        return pltpu.make_async_remote_copy(
            src_ref=src,
            dst_ref=dst,
            send_sem=x_send.at[kind, d - 1],
            recv_sem=x_recv.at[kind, d - 1],
            device_id={"dp_0": lax.rem(x + d, xs)},
            device_id_type=MESH,
        )

    def share(m, half, act_half):
        for d in range(1, xs):
            to = lax.rem(x + d, xs)
            lanes = pl.ds(pl.multiple_of(to * slab, slab), slab)
            x_copy(
                2 * half,
                d,
                stage.at[block(m, half * rows), lanes],
                cols.at[block(m, (2 * d + half) * rows)],
            ).start()
            x_copy(
                2 * half + 1,
                d,
                acts.at[block(m, act_half * rows)],
                acts.at[block(m, (2 * d + act_half) * rows)],
            ).start()

    def forward(m):
        @pl.when(jnp.logical_not(first))
        def _():
            ahead_copy(m).wait_recv()

        stream = stage[block(m), :].astype(f32)
        inv = lax.rsqrt(jnp.mean(stream * stream, axis=-1, keepdims=True) + EPSILON)
        inner = jnp.dot(stage[block(m), :], weight[...], preferred_element_type=f32)
        hidden = jnp.tanh(inner * inv).astype(bf16)
        acts[block(m, rows), :] = hidden
        inv_rms[block(m), :] = jnp.broadcast_to(inv, (STEP_ROWS, 128))

        @pl.when(jnp.logical_not(last))
        def _():
            grown = stream + jnp.dot(hidden, flip[...], preferred_element_type=f32)
            ahead[block(m), :] = grown.astype(bf16)

            @pl.when(m > 0)
            def _():
                ahead_copy(m - 1).wait_send()

            ahead_copy(m).start()

        share(m, 0, 1)

    def backward(m):
        @pl.when(jnp.logical_not(last))
        def _():
            behind_copy(m).wait_recv()

        cot = stage[block(m, rows), :]
        hidden = acts[block(m, rows), :].astype(f32)
        inv = inv_rms[block(m), 0:1]
        act_grad = jnp.dot(cot, weight[...], preferred_element_type=f32) * (1.0 - hidden * hidden)
        acts[block(m), :] = (act_grad * inv).astype(bf16)

        @pl.when(jnp.logical_not(first))
        def _():
            norm_grad = jnp.dot(act_grad.astype(bf16), flip[...], preferred_element_type=f32)
            wide = stage[block(m), :].astype(f32) * inv
            correction = jnp.mean(norm_grad * wide, axis=-1, keepdims=True)
            shrunk = cot.astype(f32) + inv * (norm_grad - wide * correction)
            behind[block(m), :] = shrunk.astype(bf16)

            @pl.when(m > 0)
            def _():
                behind_copy(m - 1).wait_send()

            behind_copy(m).start()

        share(m, 1, 0)

    lead = jnp.where(last, 1, jnp.where(section == sections - 2, 3, steps))

    def tick(t, carry):
        k = t - lead
        middle = jnp.logical_and(t >= lead, t < 2 * steps - lead)
        odd = lax.rem(k + 2 * steps, 2) == 1
        half = lax.div(k + 2 * steps, 2) - steps
        is_forward = jnp.logical_or(t < lead, jnp.logical_and(middle, odd))
        m_forward = jnp.where(t < lead, t, lead + half)
        m_backward = jnp.where(middle, half, t - steps)

        @pl.when(is_forward)
        def _():
            forward(m_forward)

        @pl.when(jnp.logical_not(is_forward))
        def _():
            backward(m_backward)

        return carry

    lax.fori_loop(0, 2 * steps, tick, 0)

    own = pl.ds(pl.multiple_of(x * slab, slab), slab)
    cols[0 : 2 * rows, :] = stage[:, own]

    def shared(kind, d):
        part = pl.ds((2 * d + (kind // 2 if kind % 2 == 0 else 1 - kind // 2)) * rows, rows)
        buffer = cols if kind % 2 == 0 else acts
        return x_copy(kind, d, buffer.at[part], buffer.at[part])

    for d in range(1, xs):
        for kind in range(4):
            shared(kind, d).wait_recv()
    local = across_rows(cols[...], acts[...])
    partial[...] = local.astype(bf16).reshape(partial.shape)

    def plane_copy(d):
        to, device = plane(d)
        return pltpu.make_async_remote_copy(
            src_ref=partial.at[to],
            dst_ref=arrived.at[d - 1],
            send_sem=plane_send.at[d - 1],
            recv_sem=plane_recv.at[d - 1],
            device_id=device,
            device_id_type=MESH,
        )

    for d in range(1, ys * zs):
        plane_copy(d).start()
    summed = partial[place].astype(f32)
    for d in range(1, ys * zs):
        plane_copy(d).wait_recv()
        summed = summed + arrived[d - 1].astype(f32)
    out[0] = summed * factor

    for d in range(1, ys * zs):
        plane_copy(d).wait_send()
    for d in range(1, xs):
        for kind in range(4):
            shared(kind, d).wait_send()

    @pl.when(jnp.logical_not(last))
    def _():
        ahead_copy(steps - 1).wait_send()

    @pl.when(jnp.logical_not(first))
    def _():
        behind_copy(steps - 1).wait_send()


def on_device(node_table, tiles, neighbours, distances, proj, upstream):
    micro, points = tiles.shape
    rows = micro * points
    _, width, rank = proj.shape
    xs, ys, zs = (lax.axis_size(a) for a in DP)
    steps = rows // STEP_ROWS
    share = width // (xs * ys * zs)
    vmem = pl.BlockSpec(memory_space=pltpu.VMEM)
    hbm = pl.BlockSpec(memory_space=pltpu.HBM)
    dma = pltpu.SemaphoreType.DMA
    return pl.pallas_call(
        functools.partial(kernel, 1.0 / math.sqrt(rows * xs * ys * zs)),
        out_shape=jax.ShapeDtypeStruct((1, share, rank), f32),
        in_specs=[vmem] * 3 + [hbm] * 3,
        out_specs=vmem,
        scratch_shapes=[
            pltpu.VMEM(node_table.shape, bf16),
            pltpu.VMEM((width, rank), bf16),
            pltpu.VMEM((rank, width), bf16),
            pltpu.VMEM((2 * rows, width), bf16),
            pltpu.VMEM((rows, width), bf16),
            pltpu.VMEM((rows, width), bf16),
            pltpu.VMEM((rows, 128), f32),
            pltpu.VMEM((2 * xs * rows, width // xs), bf16),
            pltpu.VMEM((2 * xs * rows, rank), bf16),
            pltpu.VMEM((ys * zs, share, rank), bf16),
            pltpu.VMEM((ys * zs - 1, share, rank), bf16),
            dma,
            dma((steps,)),
            dma,
            dma((steps,)),
            dma((4, xs - 1)),
            dma((4, xs - 1)),
            dma((ys * zs - 1,)),
            dma((ys * zs - 1,)),
            dma((3,)),
        ],
        compiler_params=pltpu.CompilerParams(
            collective_id=0, has_side_effects=True
        ),
    )(
        tiles,
        neighbours.transpose(0, 2, 1),
        distances.transpose(0, 2, 1),
        node_table,
        proj,
        upstream.reshape(rows, width),
    )


def solution(mesh):
    finer = Mesh(
        mesh.devices.reshape(mesh.shape["section"], 4, 2, 8), ("section", "dp_0", "dp_1", "dp_2")
    )
    in_specs = (
        P(),
        P(None, DP),
        P(None, DP, None),
        P(None, DP, None),
        P("section", None, None),
        P(None, DP, None),
    )
    out_specs = P("section", DP, None)
    return jax.shard_map(
        on_device, mesh=finer, in_specs=in_specs, out_specs=out_specs, check_vma=False
    )
```
